32 devices in a mesh: vocab: 16 (over z, y, x), pipe: 2 (over core).
Axes of the slice: x: 2, y: 2, z: 4, core: 2. Of those that a mesh axis runs over, the one named last changes fastest.
Arguments:
- hidden_a: bfloat16 [512, 4096], P('pipe', 'vocab'), parts along dimension 0, may hold values from -8 to 8, as said below
- labels_a: int32 [512], P('pipe'), parts along dimension 0, may hold values from 0 to 8191
- hidden_b: bfloat16 [512, 4096], P('pipe', 'vocab'), parts along dimension 0, may hold values from -8 to 8, as said below
- labels_b: int32 [512], P('pipe'), parts along dimension 0, may hold values from 0 to 8191
- loss_cotangent: float32 [512], P('pipe'), parts along dimension 0, may hold values from -192 to 192
- out_weight: bfloat16 [8192, 8192], P('pipe', 'vocab'), parts along dimension 0, may hold values from -0.28125 to 0.28125, as said below
Outputs:
- logits_a: bfloat16 [512, 8192], P('pipe', 'vocab'), parts along dimension 0
- loss_a: float32 [512], P('pipe'), parts along dimension 0
- amax_scale: float32 [2], P('pipe'), parts along dimension 0
- grad_hidden_b: bfloat16 [512, 4096], P('pipe', 'vocab'), parts along dimension 0
The draws below stay inside these ranges and needn't reach their ends.
There are 2 independent parts, one for each index of `pipe`. The reference program is written for one: setup_inputs(seed, part) draws one part's arguments, and reference() takes and returns one part's arrays. A program takes and returns all parts, laid end to end along the dimension named above; each array names one. Nothing has to cross between parts.
Inputs may be any that keep to these rules, and one draw needn't show every extreme that they name: `hidden_a`: hidden states of order one. `hidden_b`: hidden states of order one. `out_weight`: entries of scale 3 over the square root of 4096.
All inputs are finite; a program needn't handle non-finite values. Where the reference program divides by a largest or mean magnitude, that divisor is 1e-20 or more.
Results may differ from the reference program's by a relative error of at most 0.0048.
Values may be sent and summed in bfloat16 or wider, within the bound.
A program may use at most 64 MiB of HBM per device.

```python
import jax
import jax.numpy as jnp
from jax import lax

D = 4096
TOK_A = 256
TOK_B = 256
VOCAB = 8192


def weight_matrix(key):
    raw = jax.random.normal(jax.random.fold_in(key, 11), (D, VOCAB), jnp.float32)
    return jnp.clip(raw, -6.0, 6.0) * (3.0 / D ** 0.5)


def hidden_rows(key, count, salt):
    base = jax.random.normal(jax.random.fold_in(key, salt), (count, D), jnp.float32)
    return jnp.clip(base, -8.0, 8.0)


def draw_out_weight(key, part):
    return weight_matrix(key).astype(jnp.bfloat16)


def draw_hidden_a(key, part):
    return hidden_rows(key, TOK_A, 101).astype(jnp.bfloat16)


def draw_hidden_b(key, part):
    return hidden_rows(key, TOK_B, 211).astype(jnp.bfloat16)


def with_ends(values, key, smallest, largest):
    place = [jax.random.randint(jax.random.fold_in(key, axis), (), 0, length) for axis, length in enumerate(values.shape)]
    widest = values.shape.index(max(values.shape))
    next_to = place[:widest] + [(place[widest] + 1) % values.shape[widest]] + place[widest + 1:]
    return values.at[tuple(place)].set(smallest).at[tuple(next_to)].set(largest)


def bell_draw(own_key, extent, deviation, bound, held_as=jnp.bfloat16):
    drawn = jax.random.normal(own_key, extent, jnp.float32) * deviation
    return jnp.minimum(jnp.maximum(drawn, -bound), bound).astype(held_as)


def setup_inputs(seed: int = 0, part: int = 0) -> dict:
    arg_keys = jax.random.split(jax.random.key(seed), 7)
    part_splits = jax.random.split(jax.random.fold_in(arg_keys[6], part), 7)
    hidden_a = draw_hidden_a(jax.random.fold_in(jax.random.fold_in(arg_keys[6], part), 71), part)
    labels_a = with_ends(jax.random.randint(part_splits[1], (TOK_A,), 0, VOCAB), jax.random.fold_in(part_splits[1], 1), 0, VOCAB - 1).astype(jnp.int32)
    hidden_b = draw_hidden_b(jax.random.fold_in(jax.random.fold_in(arg_keys[6], part), 71), part)
    labels_b = with_ends(jax.random.randint(part_splits[3], (TOK_B,), 0, VOCAB), jax.random.fold_in(part_splits[3], 1), 0, VOCAB - 1).astype(jnp.int32)
    loss_cotangent = bell_draw(part_splits[4], (TOK_B,), 32.0, 192.0, jnp.float32)
    out_weight = draw_out_weight(jax.random.fold_in(jax.random.fold_in(arg_keys[6], part), 71), part)
    return dict(hidden_a=hidden_a, labels_a=labels_a, hidden_b=hidden_b, labels_b=labels_b, loss_cotangent=loss_cotangent, out_weight=out_weight)


def reference(hidden_a, labels_a, hidden_b, labels_b, loss_cotangent, out_weight):
    scores_a = jnp.dot(hidden_a, out_weight, preferred_element_type=jnp.float32)
    logits_a = scores_a.astype(jnp.bfloat16)
    peak_a = jnp.max(scores_a, axis=1)
    total_a = jnp.sum(jnp.exp(scores_a - peak_a[:, None]), axis=1)
    label_a = jnp.take_along_axis(scores_a, labels_a.astype(jnp.int32)[:, None], axis=1)[:, 0]
    loss_a = jnp.log(total_a) + peak_a - label_a
    amax_scale = (448.0 / jnp.max(jnp.abs(scores_a))).reshape(1).astype(jnp.float32)
    scores_b = jnp.dot(hidden_b, out_weight, preferred_element_type=jnp.float32)
    peak_b = jnp.max(scores_b, axis=1)
    total_b = jnp.sum(jnp.exp(scores_b - peak_b[:, None]), axis=1)
    columns = lax.broadcasted_iota(jnp.int32, scores_b.shape, 1)
    onehot = (columns == labels_b.astype(jnp.int32)[:, None]).astype(jnp.float32)
    probs = jnp.exp(scores_b - peak_b[:, None]) / total_b[:, None]
    dlogits_b = ((probs - onehot) * loss_cotangent[:, None]).astype(jnp.bfloat16)
    grad_full = lax.dot_general(dlogits_b, out_weight, (((1,), (1,)), ((), ())), preferred_element_type=jnp.float32)
    return logits_a, loss_a, amax_scale, grad_full.astype(jnp.bfloat16)
```

```python
import functools

import jax
import jax.numpy as jnp
from jax import lax
from jax.experimental import pallas as pl
from jax.experimental.pallas import tpu as pltpu
from jax.sharding import PartitionSpec as P

MESH = pl.DeviceIdType.MESH
F32 = jnp.float32
BF16 = jnp.bfloat16
QUAD = 4
LANES = 128


def to_column(row):
    return jnp.broadcast_to(row, (LANES, row.shape[1])).T[:, :1]


def to_row(column):
    return jnp.broadcast_to(column, (column.shape[0], LANES)).T[:1, :]


def kernel(
    n, ha, la, hb, lb, cot, w_hbm, logits, loss, amax, grad,
    w, ga, gb, sa, sb, dl, send, near, x1, y1, x2, y2, r3, st_a, st_b, send_sem, recv_sem, w_sem,
):
    levels = n // QUAD
    tok, width = ha.shape
    half = tok // 2
    vocab = w.shape[1]
    me = lax.axis_index("vocab")
    z, q = me // QUAD, me % QUAD
    xq = (q // 2) * 2 + 1 - q % 2
    yq = (q + 2) % QUAD
    dq = QUAD - 1 - q
    xn, yn = z * QUAD + xq, z * QUAD + yq

    w_copy = pltpu.make_async_copy(w_hbm, w, w_sem)
    w_copy.start()
    barrier = pltpu.get_barrier_semaphore()
    for off in range(1, n):
        pl.semaphore_signal(
            barrier, inc=1, device_id={"vocab": lax.rem(me + off, n)}, device_id_type=MESH
        )

    def cols(index):
        return pl.ds(pl.multiple_of(index * width, width), width)

    gb[:, cols(me)] = hb[...]
    ga[:, cols(me)] = ha[...]
    pl.semaphore_wait(barrier, n - 1)

    copies = []

    def start(src, dst, to):
        k = len(copies)
        copy = pltpu.make_async_remote_copy(
            src_ref=src, dst_ref=dst, send_sem=send_sem.at[k], recv_sem=recv_sem.at[k],
            device_id={"vocab": to}, device_id_type=MESH,
        )
        copy.start()
        copies.append(copy)
        return copy

    def level(dz):
        return lax.rem(z + levels - dz, levels)

    class Gather:
        def __init__(self, own, whole):
            self.own, self.whole = own, whole
            self.z, self.x, self.y, self.dx, self.dy = {}, {}, {}, {}, {}

        def line(self):
            for dz in seq[1:]:
                to = lax.rem(z + dz, levels) * QUAD + q
                self.z[dz] = start(self.own, self.whole.at[:, cols(me)], to)

        def plane(self, dz):
            if dz:
                self.z[dz].wait_recv()
            block = self.whole.at[:, cols(level(dz) * QUAD + q)]
            src = block if dz else self.own
            self.x[dz] = start(src, block, xn)
            self.y[dz] = start(src, block, yn)

        def relay(self, dz):
            self.x[dz].wait_recv()
            block = self.whole.at[pl.ds(0, half), cols(level(dz) * QUAD + xq)]
            self.dx[dz] = start(block, block, yn)
            self.y[dz].wait_recv()
            block = self.whole.at[pl.ds(half, half), cols(level(dz) * QUAD + yq)]
            self.dy[dz] = start(block, block, xn)

        def multiply(self, dz, scores, first):
            self.dx[dz].wait_recv()
            self.dy[dz].wait_recv()
            depth = QUAD * width
            rows = pl.ds(pl.multiple_of(level(dz) * depth, depth), depth)
            term = jnp.dot(self.whole[:, rows], w[rows, :], preferred_element_type=F32)
            scores[...] = term if first else scores[...] + term

    def spread(stats):
        return [start(stats.at[me], stats.at[me], lax.rem(me + off, n)) for off in range(1, n)]

    seq = [0] + sorted(range(1, levels), key=lambda dz: min(dz, levels - dz))
    last = seq[-1]
    b, a = Gather(hb, gb), Gather(ha, ga)
    b.line()
    b.plane(0)
    for i in range(1, levels):
        b.plane(seq[i])
        b.relay(seq[i - 1])
        if i == 1:
            w_copy.wait()
        else:
            b.multiply(seq[i - 2], sb, i == 2)
    a.line()
    b.relay(last)
    a.plane(0)
    if levels > 1:
        b.multiply(seq[-2], sb, levels == 2)
    b.multiply(last, sb, levels == 1)

    scores = sb[...]
    peak = jnp.max(scores, axis=1, keepdims=True)
    total = jnp.sum(jnp.exp(scores - peak), axis=1, keepdims=True)
    st_b[me, :, pl.ds(0, tok)] = to_row(peak)
    st_b[me, :, pl.ds(tok, tok)] = to_row(total)
    stats_b = spread(st_b)

    held = max(1, levels - 1)
    for i in range(1, held):
        a.plane(seq[i])
        if i < held - 1:
            a.relay(seq[i - 1])
        else:
            a.relay(seq[i - 1])

    for copy in stats_b:
        copy.wait_recv()
    peaks, totals = st_b[:, :, pl.ds(0, tok)], st_b[:, :, pl.ds(tok, tok)]
    peak = jnp.max(peaks, axis=0)
    total = jnp.sum(totals * jnp.exp(peaks - peak[None]), axis=0)
    peak_c, inv_c, cot_c = to_column(peak), to_column(1.0 / total), to_column(cot[...])
    columns = me * vocab + lax.broadcasted_iota(jnp.int32, (tok, vocab), 1)
    probs = jnp.exp(sb[...] - peak_c) * inv_c
    onehot = (columns == to_column(lb[...])).astype(F32)
    dl[...] = ((probs - onehot) * cot_c).astype(BF16)

    def term(index):
        rows = pl.ds(pl.multiple_of(index * width, width), width)
        return lax.dot_general(
            dl[...], w[rows, :], (((1,), (1,)), ((), ())), preferred_element_type=F32
        )

    out = [dz for dz in seq if dz] + [0]
    cx, cy = {}, {}
    for dz in out:
        slot = send.at[3 * dz]
        slot[...] = term(level(dz) * QUAD + dq).astype(BF16)
        cx[dz] = start(slot.at[pl.ds(0, half)], x1.at[dz], xn)
        cy[dz] = start(slot.at[pl.ds(half, half)], y1.at[dz], yn)
    if held >= 2:
        a.relay(seq[held - 1])
    for i in range(held, levels):
        a.plane(seq[i])
    bx, by = {}, {}
    for dz in out:
        to_x, to_y = send.at[3 * dz + 1], send.at[3 * dz + 2]
        tx = term(level(dz) * QUAD + xq)
        ty = term(level(dz) * QUAD + yq)
        cx[dz].wait_recv()
        cy[dz].wait_recv()
        to_x[pl.ds(0, half), :] = tx[:half].astype(BF16)
        to_x[pl.ds(half, half), :] = (tx[half:] + y1[dz].astype(F32)).astype(BF16)
        to_y[pl.ds(0, half), :] = (ty[:half] + x1[dz].astype(F32)).astype(BF16)
        to_y[pl.ds(half, half), :] = ty[half:].astype(BF16)
        bx[dz] = start(to_x, x2.at[dz], xn)
        by[dz] = start(to_y, y2.at[dz], yn)
    for i in range(held, levels):
        a.relay(seq[i])

    for i in range(levels):
        a.multiply(seq[i], sa, i == 0)
    scores = sa[...]
    logits[...] = scores.astype(BF16)
    peak = jnp.max(scores, axis=1, keepdims=True)
    total = jnp.sum(jnp.exp(scores - peak), axis=1, keepdims=True)
    label = jnp.sum(
        jnp.where(columns == to_column(la[...]), scores, 0.0), axis=1, keepdims=True
    )
    largest = jnp.max(jnp.abs(scores), axis=1, keepdims=True)
    for i, value in enumerate((peak, total, label, largest)):
        st_a[me, :, pl.ds(i * tok, tok)] = to_row(value)
    stats_a = spread(st_a)

    lines = {}
    for dz in out:
        near[...] = term(level(dz) * QUAD + q)
        bx[dz].wait_recv()
        by[dz].wait_recv()
        sums = near[...] + x2[dz].astype(F32) + y2[dz].astype(F32)
        if dz:
            slot = send.at[3 * levels + dz - 1]
            slot[...] = sums.astype(BF16)
            lines[dz] = start(slot, r3.at[dz - 1], level(dz) * QUAD + q)
        else:
            near[...] = sums

    for copy in stats_a:
        copy.wait_recv()
    peaks, totals = st_a[:, :, pl.ds(0, tok)], st_a[:, :, pl.ds(tok, tok)]
    peak = jnp.max(peaks, axis=0)
    total = jnp.sum(totals * jnp.exp(peaks - peak[None]), axis=0)
    label = jnp.sum(st_a[:, :, pl.ds(2 * tok, tok)], axis=0)
    loss[...] = jnp.log(total) + peak - label
    largest = jnp.max(jnp.max(st_a[:, :, pl.ds(3 * tok, tok)], axis=0), axis=1, keepdims=True)
    amax[...] = 448.0 / largest

    sums = near[...]
    for dz in out[:-1]:
        lines[dz].wait_recv()
        sums = sums + r3[dz - 1].astype(F32)
    grad[...] = sums.astype(BF16)
    for copy in copies:
        copy.wait_send()


def fused(n, hidden_a, labels_a, hidden_b, labels_b, loss_cotangent, out_weight):
    tok, width = hidden_a.shape
    depth, vocab = out_weight.shape
    levels = n // QUAD
    half = tok // 2
    sends = 3 * (5 * levels - 1) + 2 * (n - 1)
    vmem = pl.BlockSpec(memory_space=pltpu.VMEM)
    row = lambda value: value.reshape(1, tok)
    logits, loss, amax, grad = pl.pallas_call(
        functools.partial(kernel, n),
        out_shape=(
            jax.ShapeDtypeStruct((tok, vocab), BF16),
            jax.ShapeDtypeStruct((1, tok), F32),
            jax.ShapeDtypeStruct((1, 1), F32),
            jax.ShapeDtypeStruct((tok, width), BF16),
        ),
        in_specs=[vmem] * 5 + [pl.BlockSpec(memory_space=pl.ANY)],
        out_specs=(vmem,) * 4,
        scratch_shapes=[
            pltpu.VMEM((depth, vocab), BF16),
            pltpu.VMEM((tok, depth), BF16),
            pltpu.VMEM((tok, depth), BF16),
            pltpu.VMEM((tok, vocab), F32),
            pltpu.VMEM((tok, vocab), F32),
            pltpu.VMEM((tok, vocab), BF16),
            pltpu.VMEM((4 * levels - 1, tok, width), BF16),
            pltpu.VMEM((tok, width), F32),
            pltpu.VMEM((levels, half, width), BF16),
            pltpu.VMEM((levels, half, width), BF16),
            pltpu.VMEM((levels, tok, width), BF16),
            pltpu.VMEM((levels, tok, width), BF16),
            pltpu.VMEM((max(1, levels - 1), tok, width), BF16),
            pltpu.VMEM((n, 1, 4 * tok), F32),
            pltpu.VMEM((n, 1, 2 * tok), F32),
            pltpu.SemaphoreType.DMA((sends,)),
            pltpu.SemaphoreType.DMA((sends,)),
            pltpu.SemaphoreType.DMA,
        ],
        compiler_params=pltpu.CompilerParams(
            collective_id=0, has_side_effects=True, vmem_limit_bytes=48 * 1024 * 1024
        ),
    )(hidden_a, row(labels_a), hidden_b, row(labels_b), row(loss_cotangent), out_weight)
    return logits, loss.reshape(tok), amax.reshape(1), grad


def plain(n, hidden_a, labels_a, hidden_b, labels_b, loss_cotangent, out_weight):
    offset = lax.axis_index("vocab") * out_weight.shape[1]

    def accumulate(portion):
        return jnp.dot(portion, out_weight, preferred_element_type=jnp.float32)

    scores_a = accumulate(lax.all_gather(hidden_a, "vocab", axis=1, tiled=True))
    scores_b = accumulate(lax.all_gather(hidden_b, "vocab", axis=1, tiled=True))
    columns_a = offset + lax.broadcasted_iota(jnp.int32, scores_a.shape, 1)
    columns_b = offset + lax.broadcasted_iota(jnp.int32, scores_b.shape, 1)
    label_local = jnp.sum(jnp.where(columns_a == labels_a[:, None], scores_a, 0.0), axis=1)
    abs_peak = jnp.max(jnp.abs(scores_a)).reshape(1)
    peak_a, largest = lax.pmax((jnp.max(scores_a, axis=1), abs_peak), "vocab")
    own_total_a = jnp.sum(jnp.exp(scores_a - peak_a[:, None]), axis=1)
    total_a, label_a = lax.psum((own_total_a, label_local), "vocab")
    peak_b = lax.pmax(jnp.max(scores_b, axis=1), "vocab")
    exps_b = jnp.exp(scores_b - peak_b[:, None])
    total_b = lax.psum(jnp.sum(exps_b, axis=1), "vocab")
    onehot = (columns_b == labels_b[:, None]).astype(jnp.float32)
    dlogits_b = ((exps_b / total_b[:, None] - onehot) * loss_cotangent[:, None]).astype(BF16)
    grad_terms = lax.dot_general(
        dlogits_b, out_weight, (((1,), (1,)), ((), ())), preferred_element_type=jnp.float32
    )
    grad = lax.psum_scatter(grad_terms, "vocab", scatter_dimension=1, tiled=True).astype(BF16)
    return scores_a.astype(BF16), jnp.log(total_a) + peak_a - label_a, 448.0 / largest, grad


def shards(n, hidden_a, *rest):
    aligned = hidden_a.shape[0] % (2 * LANES) == 0 and hidden_a.shape[1] % LANES == 0
    form = fused if n % QUAD == 0 and aligned else plain
    return form(n, hidden_a, *rest)


def solution(mesh):
    return jax.shard_map(
        functools.partial(shards, mesh.shape["vocab"]),
        mesh=mesh,
        in_specs=(
            P("pipe", "vocab"),
            P("pipe"),
            P("pipe", "vocab"),
            P("pipe"),
            P("pipe"),
            P("pipe", "vocab"),
        ),
        out_specs=(P("pipe", "vocab"), P("pipe"), P("pipe"), P("pipe", "vocab")),
        check_vma=False,
    )
```

```python
import functools

import jax
import jax.numpy as jnp
from jax import lax
from jax.experimental import pallas as pl
from jax.experimental.pallas import tpu as pltpu
from jax.sharding import PartitionSpec as P

MESH = pl.DeviceIdType.MESH
F32 = jnp.float32
BF16 = jnp.bfloat16
QUAD = 4
LANES = 128


def to_column(row):
    return jnp.broadcast_to(row, (LANES, row.shape[1])).T[:, :1]


def to_row(column):
    return jnp.broadcast_to(column, (column.shape[0], LANES)).T[:1, :]


def flip(index, mask):
    bit, out = 1, 0
    while bit <= mask:
        out = out + lax.rem(index // bit + (mask // bit) % 2, 2) * bit
        bit *= 2
    return out + (index // bit) * bit


def kernel(
    n, ha_hbm, la_hbm, hb_hbm, lb_hbm, cot_hbm, w_hbm, logits, loss, amax, grad,
    ha, la, hb, lb, cot, w, ga, gb, sa, sb, dl, send, near, x1, y1, x2, y2, r3, st_a, st_b, send_sem, recv_sem, load_sem,
):
    levels = n // QUAD
    tok, width = ha.shape
    half = tok // 2
    vocab = w.shape[1]
    me = lax.axis_index("vocab")
    z, q = me // QUAD, me % QUAD
    xq = (q // 2) * 2 + 1 - q % 2
    yq = (q + 2) % QUAD
    dq = QUAD - 1 - q
    xn, yn = z * QUAD + xq, z * QUAD + yq

    barrier = pltpu.get_barrier_semaphore()
    peers = [flip(z, k) * QUAD + q for k in range(1, levels)] + [xn, yn]
    for peer in peers:
        pl.semaphore_signal(barrier, inc=1, device_id={"vocab": peer}, device_id_type=MESH)
    pairs = ((hb_hbm, hb), (ha_hbm, ha), (la_hbm, la), (lb_hbm, lb), (cot_hbm, cot), (w_hbm, w))
    loads = [
        pltpu.make_async_copy(src, dst, load_sem.at[i]) for i, (src, dst) in enumerate(pairs)
    ]
    for load in loads:
        load.start()

    def cols(index):
        return pl.ds(pl.multiple_of(index * width, width), width)

    loads[0].wait()
    loads[1].wait()
    pl.semaphore_wait(barrier, len(peers))

    copies = []

    def start(src, dst, to):
        k = len(copies)
        copy = pltpu.make_async_remote_copy(
            src_ref=src, dst_ref=dst, send_sem=send_sem.at[k], recv_sem=recv_sem.at[k],
            device_id={"vocab": to}, device_id_type=MESH,
        )
        copy.start()
        copies.append(copy)
        return copy

    def level(dz):
        return flip(z, dz)

    class Gather:
        def __init__(self, own, whole, first, count):
            self.own, self.whole = own.at[pl.ds(first, count)], whole
            self.all, self.front = pl.ds(first, count), pl.ds(first, count // 2)
            self.back = pl.ds(first + count // 2, count // 2)
            self.z, self.x, self.y, self.dx, self.dy = {}, {}, {}, {}, {}

        def line(self):
            for dz in seq[1:]:
                to = flip(z, dz) * QUAD + q
                self.z[dz] = start(self.own, self.whole.at[self.all, cols(me)], to)

        def plane(self, dz):
            if dz and self.z:
                self.z[dz].wait_recv()
            block = self.whole.at[self.all, cols(level(dz) * QUAD + q)]
            src = block if dz else self.own
            self.x[dz] = start(src, block, xn)
            self.y[dz] = start(src, block, yn)

        def relay(self, dz):
            self.x[dz].wait_recv()
            block = self.whole.at[self.front, cols(level(dz) * QUAD + xq)]
            self.dx[dz] = start(block, block, yn)
            self.y[dz].wait_recv()
            block = self.whole.at[self.back, cols(level(dz) * QUAD + yq)]
            self.dy[dz] = start(block, block, xn)

        def corner(self, dz):
            self.dx[dz].wait_recv()
            self.dy[dz].wait_recv()

        def lines(self, column):
            block = self.whole.at[self.all, cols(z * QUAD + column)]
            for dz in seq[1:]:
                src = self.own if column is q else block
                self.z[dz, len(self.z)] = start(src, block, flip(z, dz) * QUAD + q)

        def multiply(self, dz, scores, first):
            depth = QUAD * width
            rows = pl.ds(pl.multiple_of(level(dz) * depth, depth), depth)
            term = jnp.dot(self.whole[:, rows], w[rows, :], preferred_element_type=F32)
            scores[...] = term if first else scores[...] + term

    def spread(stats):
        return [start(stats.at[me], stats.at[me], lax.rem(me + off, n)) for off in range(1, n)]

    seq = list(range(levels))
    last = seq[-1]
    b = Gather(hb, gb, 0, tok)
    cut = tok * 7 // 8
    a = Gather(ha, ga, 0, cut)
    late = Gather(ha, ga, cut, tok - cut)
    b.plane(0)
    b.line()
    late.plane(0)
    gb[:, cols(me)] = hb[...]
    ga[:, cols(me)] = ha[...]
    for i in range(1, levels):
        b.plane(i)
        b.relay(i - 1)
        if i == 1:
            late.relay(0)
            for load in loads[2:]:
                load.wait()
        else:
            b.corner(i - 2)
            b.multiply(i - 2, sb, i == 2)
        if i == last:
            a.line()
            late.lines(q)
            late.lines(xq)
            late.lines(yq)
            late.corner(0)
            late.lines(dq)
    b.relay(last)

    order = [functools.partial(a.plane, 0)]
    for i in range(1, levels):
        order += [functools.partial(a.plane, i), functools.partial(a.relay, i - 1)]
    order.append(functools.partial(a.relay, last))

    def advance(count):
        for step in order[:count]:
            step()
        del order[:count]

    advance(2)
    for i in range(max(0, levels - 2), levels):
        b.corner(i)
        b.multiply(i, sb, i == 0)

    scores = sb[...]
    peak = jnp.max(scores, axis=1, keepdims=True)
    total = jnp.sum(jnp.exp(scores - peak), axis=1, keepdims=True)
    st_b[me, :, pl.ds(0, tok)] = to_row(peak)
    st_b[me, :, pl.ds(tok, tok)] = to_row(total)
    stats_b = spread(st_b)

    advance(4)
    for copy in stats_b:
        copy.wait_recv()
    peaks, totals = st_b[:, :, pl.ds(0, tok)], st_b[:, :, pl.ds(tok, tok)]
    peak = jnp.max(peaks, axis=0)
    total = jnp.sum(totals * jnp.exp(peaks - peak[None]), axis=0)
    peak_c, inv_c, cot_c = to_column(peak), to_column(1.0 / total), to_column(cot[...])
    columns = me * vocab + lax.broadcasted_iota(jnp.int32, (tok, vocab), 1)
    probs = jnp.exp(sb[...] - peak_c) * inv_c
    onehot = (columns == to_column(lb[...])).astype(F32)
    dl[...] = ((probs - onehot) * cot_c).astype(BF16)

    def term(index):
        rows = pl.ds(pl.multiple_of(index * width, width), width)
        return lax.dot_general(
            dl[...], w[rows, :], (((1,), (1,)), ((), ())), preferred_element_type=F32
        )

    out = seq[::-1]
    cx, cy = {}, {}
    for dz in out:
        slot = send.at[3 * dz]
        slot[...] = term(level(dz) * QUAD + dq).astype(BF16)
        cx[dz] = start(slot.at[pl.ds(0, half)], x1.at[dz], xn)
        cy[dz] = start(slot.at[pl.ds(half, half)], y1.at[dz], yn)
    advance(len(order))
    bx, by = {}, {}
    for dz in out:
        to_x, to_y = send.at[3 * dz + 1], send.at[3 * dz + 2]
        tx = term(level(dz) * QUAD + xq)
        ty = term(level(dz) * QUAD + yq)
        cx[dz].wait_recv()
        cy[dz].wait_recv()
        to_x[pl.ds(0, half), :] = tx[:half].astype(BF16)
        to_x[pl.ds(half, half), :] = (tx[half:] + y1[dz].astype(F32)).astype(BF16)
        to_y[pl.ds(0, half), :] = (ty[:half] + x1[dz].astype(F32)).astype(BF16)
        to_y[pl.ds(half, half), :] = ty[half:].astype(BF16)
        bx[dz] = start(to_x, x2.at[dz], xn)
        by[dz] = start(to_y, y2.at[dz], yn)

    def finish_a(step):
        a.corner(step)
        for key, copy in late.z.items():
            if key[0] == step:
                copy.wait_recv()
        a.multiply(step, sa, step == 0)

    lines = {}
    seen = 0
    for turn, dz in enumerate(out):
        if turn == len(out) - 1:
            for i in range(seen, levels):
                finish_a(i)
            scores = sa[...]
            logits[...] = scores.astype(BF16)
            peak = jnp.max(scores, axis=1, keepdims=True)
            total = jnp.sum(jnp.exp(scores - peak), axis=1, keepdims=True)
            label = jnp.sum(
                jnp.where(columns == to_column(la[...]), scores, 0.0), axis=1, keepdims=True
            )
            largest = jnp.max(jnp.abs(scores), axis=1, keepdims=True)
            for i, value in enumerate((peak, total, label, largest)):
                st_a[me, :, pl.ds(i * tok, tok)] = to_row(value)
            stats_a = spread(st_a)

        elif turn:
            for i in range(seen, min(seen + 2, levels)):
                finish_a(i)
            seen = min(seen + 2, levels)
        near[...] = term(level(dz) * QUAD + q)
        bx[dz].wait_recv()
        by[dz].wait_recv()
        sums = near[...] + x2[dz].astype(F32) + y2[dz].astype(F32)
        if dz:
            slot = send.at[3 * levels + dz - 1]
            slot[...] = sums.astype(BF16)
            lines[dz] = start(slot, r3.at[dz - 1], level(dz) * QUAD + q)
        else:
            near[...] = sums

    for copy in stats_a:
        copy.wait_recv()
    peaks, totals = st_a[:, :, pl.ds(0, tok)], st_a[:, :, pl.ds(tok, tok)]
    peak = jnp.max(peaks, axis=0)
    total = jnp.sum(totals * jnp.exp(peaks - peak[None]), axis=0)
    label = jnp.sum(st_a[:, :, pl.ds(2 * tok, tok)], axis=0)
    loss[...] = jnp.log(total) + peak - label
    largest = jnp.max(jnp.max(st_a[:, :, pl.ds(3 * tok, tok)], axis=0), axis=1, keepdims=True)
    amax[...] = 448.0 / largest

    sums = near[...]
    for dz in out[:-1]:
        lines[dz].wait_recv()
        sums = sums + r3[dz - 1].astype(F32)
    grad[...] = sums.astype(BF16)
    for copy in copies:
        copy.wait_send()


def fused(n, hidden_a, labels_a, hidden_b, labels_b, loss_cotangent, out_weight):
    tok, width = hidden_a.shape
    depth, vocab = out_weight.shape
    levels = n // QUAD
    half = tok // 2
    sends = 3 * (5 * levels - 1) + 2 * (n - 1) + 4 + 4 * (levels - 1)
    vmem = pl.BlockSpec(memory_space=pltpu.VMEM)
    row = lambda value: value.reshape(1, tok)
    logits, loss, amax, grad = pl.pallas_call(
        functools.partial(kernel, n),
        out_shape=(
            jax.ShapeDtypeStruct((tok, vocab), BF16),
            jax.ShapeDtypeStruct((1, tok), F32),
            jax.ShapeDtypeStruct((1, 1), F32),
            jax.ShapeDtypeStruct((tok, width), BF16),
        ),
        in_specs=[pl.BlockSpec(memory_space=pltpu.HBM)] * 6,
        out_specs=(vmem,) * 4,
        scratch_shapes=[
            pltpu.VMEM((tok, width), BF16),
            pltpu.VMEM((1, tok), jnp.int32),
            pltpu.VMEM((tok, width), BF16),
            pltpu.VMEM((1, tok), jnp.int32),
            pltpu.VMEM((1, tok), F32),
            pltpu.VMEM((depth, vocab), BF16),
            pltpu.VMEM((tok, depth), BF16),
            pltpu.VMEM((tok, depth), BF16),
            pltpu.VMEM((tok, vocab), F32),
            pltpu.VMEM((tok, vocab), F32),
            pltpu.VMEM((tok, vocab), BF16),
            pltpu.VMEM((4 * levels - 1, tok, width), BF16),
            pltpu.VMEM((tok, width), F32),
            pltpu.VMEM((levels, half, width), BF16),
            pltpu.VMEM((levels, half, width), BF16),
            pltpu.VMEM((levels, tok, width), BF16),
            pltpu.VMEM((levels, tok, width), BF16),
            pltpu.VMEM((max(1, levels - 1), tok, width), BF16),
            pltpu.VMEM((n, 1, 4 * tok), F32),
            pltpu.VMEM((n, 1, 2 * tok), F32),
            pltpu.SemaphoreType.DMA((sends,)),
            pltpu.SemaphoreType.DMA((sends,)),
            pltpu.SemaphoreType.DMA((6,)),
        ],
        compiler_params=pltpu.CompilerParams(
            collective_id=0, has_side_effects=True, vmem_limit_bytes=67_043_328
        ),
    )(hidden_a, row(labels_a), hidden_b, row(labels_b), row(loss_cotangent), out_weight)
    return logits, loss.reshape(tok), amax.reshape(1), grad


def plain(n, hidden_a, labels_a, hidden_b, labels_b, loss_cotangent, out_weight):
    offset = lax.axis_index("vocab") * out_weight.shape[1]

    def accumulate(portion):
        return jnp.dot(portion, out_weight, preferred_element_type=jnp.float32)

    scores_a = accumulate(lax.all_gather(hidden_a, "vocab", axis=1, tiled=True))
    scores_b = accumulate(lax.all_gather(hidden_b, "vocab", axis=1, tiled=True))
    columns_a = offset + lax.broadcasted_iota(jnp.int32, scores_a.shape, 1)
    columns_b = offset + lax.broadcasted_iota(jnp.int32, scores_b.shape, 1)
    label_local = jnp.sum(jnp.where(columns_a == labels_a[:, None], scores_a, 0.0), axis=1)
    abs_peak = jnp.max(jnp.abs(scores_a)).reshape(1)
    peak_a, largest = lax.pmax((jnp.max(scores_a, axis=1), abs_peak), "vocab")
    own_total_a = jnp.sum(jnp.exp(scores_a - peak_a[:, None]), axis=1)
    total_a, label_a = lax.psum((own_total_a, label_local), "vocab")
    peak_b = lax.pmax(jnp.max(scores_b, axis=1), "vocab")
    exps_b = jnp.exp(scores_b - peak_b[:, None])
    total_b = lax.psum(jnp.sum(exps_b, axis=1), "vocab")
    onehot = (columns_b == labels_b[:, None]).astype(jnp.float32)
    dlogits_b = ((exps_b / total_b[:, None] - onehot) * loss_cotangent[:, None]).astype(BF16)
    grad_terms = lax.dot_general(
        dlogits_b, out_weight, (((1,), (1,)), ((), ())), preferred_element_type=jnp.float32
    )
    grad = lax.psum_scatter(grad_terms, "vocab", scatter_dimension=1, tiled=True).astype(BF16)
    return scores_a.astype(BF16), jnp.log(total_a) + peak_a - label_a, 448.0 / largest, grad


def shards(n, hidden_a, *rest):
    aligned = hidden_a.shape[0] % (2 * LANES) == 0 and hidden_a.shape[1] % LANES == 0
    levels = n // QUAD
    staged = n % QUAD == 0 and levels > 1 and levels & (levels - 1) == 0
    form = fused if staged and aligned else plain
    return form(n, hidden_a, *rest)


def solution(mesh):
    return jax.shard_map(
        functools.partial(shards, mesh.shape["vocab"]),
        mesh=mesh,
        in_specs=(
            P("pipe", "vocab"),
            P("pipe"),
            P("pipe", "vocab"),
            P("pipe"),
            P("pipe"),
            P("pipe", "vocab"),
        ),
        out_specs=(P("pipe", "vocab"), P("pipe"), P("pipe"), P("pipe", "vocab")),
        check_vma=False,
    )
```
